8 devices in a mesh: vp: 8 (over z, y, x, core).
Axes of the slice: x: 2, y: 2, z: 1, core: 2. Of those that a mesh axis runs over, the one named last changes fastest.
Arguments:
- hidden: bfloat16 [32, 2048], replicated
- ln_weight: bfloat16 [2048], replicated
- ln_bias: bfloat16 [2048], replicated
- embedding: bfloat16 [250880, 2048], P('vp')
- temperature: float32 [], replicated
- cand_ids: int32 [32, 128], replicated
Outputs:
- output 1: float32 [32, 250880], P(None, 'vp')
- output 2: float32 [32, 128], replicated
All inputs are finite; a program needn't handle non-finite values.
Results may differ from the reference program's by a relative error of at most 0.001.
Values sent between devices are 32-bit elements.
A program may use at most 1 GiB of HBM per device.

```python
import jax
import jax.numpy as jnp
from jax import lax

BATCH = 32
HIDDEN = 2048
VOCAB = 250880
CANDS = 128
CLUSTER_IDS = VOCAB // 64


def hot_scales(key_rows):
    hot_draw = jax.random.randint(key_rows, (VOCAB,), 0, 64)
    return jnp.where(hot_draw == 0, 3.0, 1.0).astype(jnp.float32)


def draw_candidates(key_cand):
    k_center, k_pick, k_offset, k_spread = jax.random.split(key_cand, 4)
    centers = jax.random.randint(k_center, (3,), 0, VOCAB - CLUSTER_IDS)
    pick_idx = jax.random.randint(k_pick, (BATCH, CANDS), 0, 3)
    offsets = jax.random.randint(k_offset, (BATCH, CANDS), 0, CLUSTER_IDS)
    spread = jax.random.randint(k_spread, (BATCH, CANDS), 0, VOCAB)
    clustered = jnp.take(centers, pick_idx) + offsets
    column = jnp.arange(CANDS)[None, :]
    cand_ids = jnp.where(column % 4 == 3, spread, clustered)
    cand_ids = cand_ids.at[0, 0].set(0).at[BATCH - 1, CANDS - 1].set(VOCAB - 1)
    return cand_ids.astype(jnp.int32)


def setup_inputs(seed: int = 0) -> dict:
    root_key = jax.random.key(seed)
    k_hidden, k_weight, k_bias, k_embed, k_hot, k_temp, k_cand = jax.random.split(root_key, 7)
    hidden = jax.random.normal(k_hidden, (BATCH, HIDDEN), jnp.float32)
    ln_weight = 1.0 + 0.5 * jax.random.normal(k_weight, (HIDDEN,), jnp.float32)
    ln_bias = 0.5 * jax.random.normal(k_bias, (HIDDEN,), jnp.float32)
    row_gain = hot_scales(k_hot) * (HIDDEN ** -0.5)
    embedding = jax.random.normal(k_embed, (VOCAB, HIDDEN), jnp.float32) * row_gain[:, None]
    temperature = jax.random.uniform(k_temp, (), jnp.float32, minval=0.8, maxval=1.25)
    return {
        "hidden": hidden.astype(jnp.bfloat16),
        "ln_weight": ln_weight.astype(jnp.bfloat16),
        "ln_bias": ln_bias.astype(jnp.bfloat16),
        "embedding": embedding.astype(jnp.bfloat16),
        "temperature": temperature,
        "cand_ids": draw_candidates(k_cand),
    }


def reference(hidden, ln_weight, ln_bias, embedding, temperature, cand_ids):
    hidden_f32 = hidden.astype(jnp.float32)
    row_mean = jnp.mean(hidden_f32, axis=-1, keepdims=True)
    centered = hidden_f32 - row_mean
    row_var = jnp.mean(centered * centered, axis=-1, keepdims=True)
    scaled = centered * lax.rsqrt(row_var + 1e-5)
    normed = (scaled * ln_weight.astype(jnp.float32) + ln_bias.astype(jnp.float32)).astype(jnp.bfloat16)
    logits = lax.dot_general(normed, embedding, (((1,), (1,)), ((), ())), preferred_element_type=jnp.float32) / temperature
    row_max = jnp.max(logits, axis=1, keepdims=True)
    exp_sum = jnp.sum(jnp.exp(logits - row_max), axis=1, keepdims=True)
    logprobs = logits - (row_max + jnp.log(exp_sum))
    cand_lp = jnp.take_along_axis(logprobs, cand_ids, axis=1)
    return logprobs, cand_lp
```

```python
import functools

import jax
import jax.numpy as jnp
from jax import lax
from jax.experimental import pallas as pl
from jax.experimental.pallas import tpu as pltpu
from jax.sharding import PartitionSpec as P

LANES = 128
TILE = 256
CHUNK = 2048
SLOTS = 4
PIECE = 4480
OFFSETS = [(1, 1, 0), (1, 1, 1), (1, 0, 0), (1, 0, 1), (0, 1, 0), (0, 1, 1), (0, 0, 1)]


def peers_of(me):
    y, x, core = me // 4, lax.rem(me // 2, 2), lax.rem(me, 2)
    return [lax.rem(y + dy, 2) * 4 + lax.rem(x + dx, 2) * 2 + lax.rem(core + dc, 2) for dy, dx, dc in OFFSETS]


def stream_kernel(axis, rows, x_ref, w_ref, b_ref, t_ref, cand_ref, emb_ref, z_ref, norm_ref, candz_ref,
                  ebuf, a_ref, m_ref, s_ref, q_ref, q_recv, st_send, st_recv,
                  ecopy_sem, q_send_sem, q_recv_sem, st_send_sem, st_recv_sem):
    me = lax.axis_index(axis)
    peers = peers_of(me)
    barrier = pltpu.get_barrier_semaphore()
    for peer in peers:
        pl.semaphore_signal(barrier, inc=1, device_id=(peer,), device_id_type=pl.DeviceIdType.MESH)

    full = rows // CHUNK
    tail = rows - full * CHUNK

    def fetch(i, slot, size=CHUNK):
        return pltpu.make_async_copy(
            emb_ref.at[pl.ds(i * CHUNK, size), :], ebuf.at[slot, pl.ds(0, size), :], ecopy_sem.at[slot])

    for i in range(SLOTS - 1):
        fetch(i, i).start()

    x = x_ref[...].astype(jnp.float32)
    centered = x - jnp.mean(x, axis=-1, keepdims=True)
    var = jnp.mean(centered * centered, axis=-1, keepdims=True)
    scaled = centered * lax.rsqrt(var + 1e-5)
    a_ref[...] = (scaled * w_ref[...].astype(jnp.float32) + b_ref[...].astype(jnp.float32)).astype(jnp.bfloat16)
    m_ref[...] = jnp.full(m_ref.shape, -jnp.inf, jnp.float32)
    s_ref[...] = jnp.zeros(s_ref.shape, jnp.float32)
    q_ref[...] = jnp.zeros(q_ref.shape, jnp.float32)
    temp = t_ref[0]

    def logits(i, slot, size=CHUNK):
        base = i * CHUNK
        for t in range(0, size, TILE):
            n = min(TILE, size - t)
            z = lax.dot_general(a_ref[...], ebuf[slot, t:t + n, :], (((1,), (1,)), ((), ())),
                                preferred_element_type=jnp.float32) / temp
            z_ref[:, pl.ds(pl.multiple_of(base + t, LANES), n)] = z

    def statistics(i, size=CHUNK):
        base = i * CHUNK
        cand = cand_ref[...] - me * rows - base
        lane, group = jnp.bitwise_and(cand, LANES - 1), jnp.right_shift(cand, 7)
        tiles = [z_ref[:, pl.ds(pl.multiple_of(base + t, LANES), LANES)] for t in range(0, size, LANES)]
        old = m_ref[...]
        new = functools.reduce(jnp.maximum, tiles, old)
        total = s_ref[...] * jnp.exp(old - new)
        q = q_ref[...]
        for k, z in enumerate(tiles):
            total = total + jnp.exp(z - new)
            q = jnp.where(group == k, jnp.take_along_axis(z, lane, axis=1, mode="promise_in_bounds"), q)
        m_ref[...] = new
        s_ref[...] = total
        q_ref[...] = q

    fetch(SLOTS - 1, SLOTS - 1).start()
    fetch(0, 0).wait()
    logits(0, 0)

    @pl.loop(1, full - SLOTS + 1)
    def _(i):
        fetch(i + SLOTS - 1, lax.rem(i + SLOTS - 1, SLOTS)).start()
        fetch(i, lax.rem(i, SLOTS)).wait()
        statistics(i - 1)
        logits(i, lax.rem(i, SLOTS))

    fetch(full, full % SLOTS, tail).start()

    @pl.loop(full - SLOTS + 1, full)
    def _(i):
        fetch(i, lax.rem(i, SLOTS)).wait()
        statistics(i - 1)
        logits(i, lax.rem(i, SLOTS))

    fetch(full, full % SLOTS, tail).wait()
    statistics(full - 1)
    logits(full, full % SLOTS, tail)
    statistics(full, tail)

    m = m_ref[...]
    row_max = jnp.max(m, axis=1, keepdims=True)
    row_sum = jnp.sum(s_ref[...] * jnp.exp(m - row_max), axis=1, keepdims=True)
    local = row_max + jnp.log(row_sum)
    diagonal = lax.broadcasted_iota(jnp.int32, m.shape, 0) == lax.broadcasted_iota(jnp.int32, m.shape, 1)
    packed = jnp.sum(jnp.where(diagonal, local, 0.0), axis=0, keepdims=True)
    st_send[...] = packed
    st_recv[me] = packed

    pl.semaphore_wait(barrier, len(peers))
    copies = []
    for k, peer in enumerate(peers):
        where = dict(device_id=(peer,), device_id_type=pl.DeviceIdType.MESH)
        copies.append((
            pltpu.make_async_remote_copy(src_ref=q_ref, dst_ref=q_recv.at[k], send_sem=q_send_sem.at[k],
                                         recv_sem=q_recv_sem.at[k], **where),
            pltpu.make_async_remote_copy(src_ref=st_send, dst_ref=st_recv.at[me], send_sem=st_send_sem.at[k],
                                         recv_sem=st_recv_sem.at[k], **where)))
    for q_copy, st_copy in copies:
        st_copy.start()
    for q_copy, st_copy in copies:
        q_copy.start()
    for q_copy, st_copy in copies:
        st_copy.wait()
    parts = [st_recv[p] for p in range(8)]
    top = functools.reduce(jnp.maximum, parts)
    norm = top + jnp.log(functools.reduce(jnp.add, [jnp.exp(p - top) for p in parts]))
    norm = jnp.sum(jnp.where(diagonal, norm, 0.0), axis=1, keepdims=True)
    norm_ref[...] = jnp.broadcast_to(norm, norm_ref.shape)
    q = q_ref[...]
    for k, (q_copy, st_copy) in enumerate(copies):
        q_copy.wait()
        q = q + q_recv[k]
    candz_ref[...] = q


def finish_kernel(z_ref, norm_ref, candz_ref, lp_ref, q_ref, buf, sem):
    norm = norm_ref[...]
    columns = z_ref.shape[1]
    copies = []
    for n, start in enumerate(range(0, columns, PIECE)):
        for c in range(start, start + PIECE, LANES):
            buf[:, c:c + LANES] = z_ref[:, c:c + LANES] - norm
        copies.append(pltpu.make_async_copy(buf.at[:, pl.ds(start, PIECE)], lp_ref.at[:, pl.ds(start, PIECE)], sem.at[n]))
        copies[-1].start()
    q_ref[...] = candz_ref[...] - norm
    for copy in copies:
        copy.wait()


def solution(mesh):
    axis = mesh.axis_names[0]

    def per_device(hidden, ln_weight, ln_bias, emb, temperature, cand_ids):
        batch, width = hidden.shape
        rows = emb.shape[0]
        vmem = pl.BlockSpec(memory_space=pltpu.VMEM)
        f32 = jnp.float32
        dma = pltpu.SemaphoreType.DMA
        z, norm, candz = pl.pallas_call(
            functools.partial(stream_kernel, axis, rows),
            out_shape=(pltpu.VMEM((batch, rows), f32), pltpu.VMEM((batch, LANES), f32),
                       pltpu.VMEM((batch, LANES), f32)),
            in_specs=[vmem, vmem, vmem, pl.BlockSpec(memory_space=pltpu.SMEM), vmem,
                      pl.BlockSpec(memory_space=pl.ANY)],
            out_specs=(vmem, vmem, vmem),
            scratch_shapes=[
                pltpu.VMEM((SLOTS, CHUNK, width), jnp.bfloat16),
                pltpu.VMEM((batch, width), jnp.bfloat16),
                pltpu.VMEM((batch, LANES), f32),
                pltpu.VMEM((batch, LANES), f32),
                pltpu.VMEM((batch, LANES), f32),
                pltpu.VMEM((7, batch, LANES), f32),
                pltpu.VMEM((1, LANES), f32),
                pltpu.VMEM((8, 1, LANES), f32),
                dma((SLOTS,)), dma((7,)), dma((7,)), dma((7,)), dma((7,)),
            ],
            compiler_params=pltpu.CompilerParams(
                collective_id=0, has_side_effects=True, vmem_limit_bytes=44 * 1024 * 1024),
        )(hidden, ln_weight.reshape(1, width), ln_bias.reshape(1, width), temperature.reshape(1), cand_ids, emb)
        return pl.pallas_call(
            finish_kernel,
            out_shape=(jax.ShapeDtypeStruct((batch, rows), f32), jax.ShapeDtypeStruct((batch, LANES), f32)),
            in_specs=[vmem, vmem, vmem],
            out_specs=(pl.BlockSpec(memory_space=pl.ANY), vmem),
            scratch_shapes=[pltpu.VMEM((batch, rows), f32), dma((rows // PIECE,))],
            compiler_params=pltpu.CompilerParams(vmem_limit_bytes=16 * 1024 * 1024),
        )(z, norm, candz)

    return jax.shard_map(
        per_device,
        mesh=mesh,
        in_specs=(P(), P(), P(), P(axis, None), P(), P()),
        out_specs=(P(None, axis), P()),
        check_vma=False,
    )
```

```python
import functools

import jax
import jax.numpy as jnp
from jax import lax
from jax.experimental import pallas as pl
from jax.experimental.pallas import tpu as pltpu
from jax.sharding import PartitionSpec as P

LANES = 128
CHUNK = 896
SLOTS = 8
DOTS = ((0, 256, False), (256, 256, True), (512, 128, False), (640, 256, True))
PIECES = (896, 1792, 3584, 6272, 6272, 6272, 6272)
OFFSETS = [(1, 1, 0), (1, 1, 1), (1, 0, 0), (1, 0, 1), (0, 1, 0), (0, 1, 1), (0, 0, 1)]
MESH = pl.DeviceIdType.MESH


def peers_of(me):
    y, x, core = me // 4, lax.rem(me // 2, 2), lax.rem(me, 2)
    return [lax.rem(y + dy, 2) * 4 + lax.rem(x + dx, 2) * 2 + lax.rem(core + dc, 2) for dy, dx, dc in OFFSETS]


def stream_kernel(axis, rows, t_ref, x_hbm, w_hbm, b_hbm, cand_hbm, emb_hbm, z_ref, norm_ref, candz_ref,
                  ebuf, et_ref, x_ref, w_ref, b_ref, cand_ref, a_ref, m_ref, s_ref, msg_ref, recv_ref,
                  ecopy_sem, in_sem, send_sem, recv_sem):
    batch, width = x_ref.shape
    chunks = rows // CHUNK
    inputs = [pltpu.make_async_copy(src, dst, in_sem.at[n]) for n, (src, dst) in enumerate(
        [(x_hbm, x_ref), (w_hbm, w_ref), (b_hbm, b_ref), (cand_hbm, cand_ref)])]
    for copy in inputs:
        copy.start()

    def fetch(i, slot):
        return pltpu.make_async_copy(emb_hbm.at[pl.ds(i * CHUNK, CHUNK), :], ebuf.at[slot], ecopy_sem.at[slot])

    for i in range(SLOTS):
        fetch(i, i).start()

    me = lax.axis_index(axis)
    peers = peers_of(me)
    barrier = pltpu.get_barrier_semaphore()
    for peer in peers:
        pl.semaphore_signal(barrier, inc=1, device_id=(peer,), device_id_type=MESH)

    for copy in inputs:
        copy.wait()
    x = x_ref[...].astype(jnp.float32)
    centered = x - jnp.mean(x, axis=-1, keepdims=True)
    var = jnp.mean(centered * centered, axis=-1, keepdims=True)
    scaled = centered * lax.rsqrt(var + 1e-5)
    gain, bias = w_ref[...].astype(jnp.float32), b_ref[...].astype(jnp.float32)
    for k in range(width // LANES):
        part = scaled[:, k * LANES:(k + 1) * LANES] * gain[k:k + 1, :] + bias[k:k + 1, :]
        a_ref[:, k * LANES:(k + 1) * LANES] = part.astype(jnp.bfloat16)
    m_ref[...] = jnp.full(m_ref.shape, -jnp.inf, jnp.float32)
    s_ref[...] = jnp.zeros(s_ref.shape, jnp.float32)
    msg_ref[...] = jnp.zeros(msg_ref.shape, jnp.float32)
    temp = t_ref[0]

    def logits(i, slot):
        for n, (first, size, flip) in enumerate(DOTS):
            tile = ebuf[slot, first:first + size, :]
            if flip:
                et_ref[n, :, :size] = tile.T
                z = jnp.dot(a_ref[...], et_ref[n, :, :size], preferred_element_type=jnp.float32)
            else:
                z = lax.dot_general(tile, a_ref[...], (((1,), (1,)), ((), ())), preferred_element_type=jnp.float32).T
            z_ref[:, pl.ds(pl.multiple_of(i * CHUNK + first, LANES), size)] = z / temp

    def statistics(i):
        cand = cand_ref[...] - me * rows - i * CHUNK
        lane, group = jnp.bitwise_and(cand, LANES - 1), jnp.right_shift(cand, 7)
        tiles = [z_ref[:, pl.ds(pl.multiple_of(i * CHUNK + t, LANES), LANES)] for t in range(0, CHUNK, LANES)]
        old = m_ref[...]
        new = functools.reduce(jnp.maximum, tiles, old)
        total = s_ref[...] * jnp.exp(old - new)
        q = msg_ref[:batch, :]
        for k, z in enumerate(tiles):
            total = total + jnp.exp(z - new)
            q = jnp.where(group == k, jnp.take_along_axis(z, lane, axis=1, mode="promise_in_bounds"), q)
        m_ref[...] = new
        s_ref[...] = total
        msg_ref[:batch, :] = q

    fetch(0, 0).wait()
    logits(0, 0)

    @pl.loop(1, chunks)
    def _(i):
        @pl.when(i + SLOTS - 1 < chunks)
        def _():
            fetch(i + SLOTS - 1, lax.rem(i + SLOTS - 1, SLOTS)).start()

        fetch(i, lax.rem(i, SLOTS)).wait()
        statistics(i - 1)
        logits(i, lax.rem(i, SLOTS))

    statistics(chunks - 1)
    m = m_ref[...]
    row_max = jnp.max(m, axis=1, keepdims=True)
    local = row_max + jnp.log(jnp.sum(s_ref[...] * jnp.exp(m - row_max), axis=1, keepdims=True))
    diagonal = lax.broadcasted_iota(jnp.int32, m.shape, 0) == lax.broadcasted_iota(jnp.int32, m.shape, 1)
    mine = jnp.sum(jnp.where(diagonal, local, 0.0), axis=0, keepdims=True)
    msg_ref[batch:batch + 1, :] = mine

    pl.semaphore_wait(barrier, len(peers))
    copies = [pltpu.make_async_remote_copy(
        src_ref=msg_ref, dst_ref=recv_ref.at[k], send_sem=send_sem.at[k], recv_sem=recv_sem.at[k],
        device_id=(peer,), device_id_type=MESH) for k, peer in enumerate(peers)]
    for copy in copies:
        copy.start()
    for copy in copies:
        copy.wait()
    parts = [mine] + [recv_ref[k, batch:batch + 1, :] for k in range(len(peers))]
    top = functools.reduce(jnp.maximum, parts)
    norm = top + jnp.log(functools.reduce(jnp.add, [jnp.exp(p - top) for p in parts]))
    norm = jnp.sum(jnp.where(diagonal, norm, 0.0), axis=1, keepdims=True)
    norm_ref[...] = jnp.broadcast_to(norm, norm_ref.shape)
    candz_ref[...] = functools.reduce(jnp.add, [recv_ref[k, :batch, :] for k in range(len(peers))], msg_ref[:batch, :])


def finish_kernel(z_ref, norm_ref, candz_ref, lp_hbm, q_ref, buf, sem):
    norm = norm_ref[...]
    copies, start = [], 0
    for n, size in enumerate(PIECES):
        for c in range(start, start + size, LANES):
            buf[:, c:c + LANES] = z_ref[:, c:c + LANES] - norm
        copies.append(pltpu.make_async_copy(buf.at[:, pl.ds(start, size)], lp_hbm.at[:, pl.ds(start, size)], sem.at[n]))
        copies[-1].start()
        start += size
    q_ref[...] = candz_ref[...] - norm
    for copy in copies:
        copy.wait()


def solution(mesh):
    axis = mesh.axis_names[0]

    def per_device(hidden, ln_weight, ln_bias, emb, temperature, cand_ids):
        batch, width = hidden.shape
        rows = emb.shape[0]
        vmem = pl.BlockSpec(memory_space=pltpu.VMEM)
        hbm = pl.BlockSpec(memory_space=pl.ANY)
        f32, bf16 = jnp.float32, jnp.bfloat16
        dma = pltpu.SemaphoreType.DMA
        block = (width // LANES, LANES)
        small = [hidden, ln_weight.reshape(block), ln_bias.reshape(block), cand_ids]
        small = [pltpu.with_memory_space_constraint(v, pltpu.HBM) for v in small]
        z, norm, candz = pl.pallas_call(
            functools.partial(stream_kernel, axis, rows),
            out_shape=(pltpu.VMEM((batch, rows), f32), pltpu.VMEM((batch, LANES), f32),
                       pltpu.VMEM((batch, LANES), f32)),
            in_specs=[pl.BlockSpec(memory_space=pltpu.SMEM)] + [hbm] * 5,
            out_specs=(vmem, vmem, vmem),
            scratch_shapes=[
                pltpu.VMEM((SLOTS, CHUNK, width), bf16),
                pltpu.VMEM((len(DOTS), width, 256), bf16),
                pltpu.VMEM((batch, width), bf16),
                pltpu.VMEM(block, bf16),
                pltpu.VMEM(block, bf16),
                pltpu.VMEM((batch, LANES), jnp.int32),
                pltpu.VMEM((batch, width), bf16),
                pltpu.VMEM((batch, LANES), f32),
                pltpu.VMEM((batch, LANES), f32),
                pltpu.VMEM((batch + 8, LANES), f32),
                pltpu.VMEM((len(OFFSETS), batch + 8, LANES), f32),
                dma((SLOTS,)), dma((4,)), dma((7,)), dma((7,)),
            ],
            compiler_params=pltpu.CompilerParams(
                collective_id=0, has_side_effects=True, vmem_limit_bytes=48 * 1024 * 1024),
        )(temperature.reshape(1), *small, emb)
        return pl.pallas_call(
            finish_kernel,
            out_shape=(jax.ShapeDtypeStruct((batch, rows), f32), jax.ShapeDtypeStruct((batch, LANES), f32)),
            in_specs=[vmem, vmem, vmem],
            out_specs=(hbm, vmem),
            scratch_shapes=[pltpu.VMEM((batch, rows), f32), dma((len(PIECES),))],
            compiler_params=pltpu.CompilerParams(vmem_limit_bytes=16 * 1024 * 1024),
        )(z, norm, candz)

    return jax.shard_map(
        per_device,
        mesh=mesh,
        in_specs=(P(), P(), P(), P(axis, None), P(), P()),
        out_specs=(P(None, axis), P()),
        check_vma=False,
    )
```

```python
import functools

import jax
import jax.numpy as jnp
from jax import lax
from jax.experimental import pallas as pl
from jax.experimental.pallas import tpu as pltpu
from jax.sharding import PartitionSpec as P

LANES = 128
CHUNK = 896
SLOTS = 5
DOTS = ((0, 128, False), (128, 256, False), (384, 256, True), (640, 256, True))
PIECES = (896, 1792, 3584, 6272, 6272, 6272, 6272)
OFFSETS = [(1, 1, 0), (1, 1, 1), (1, 0, 0), (1, 0, 1), (0, 1, 0), (0, 1, 1), (0, 0, 1)]
MESH = pl.DeviceIdType.MESH


def peers_of(me):
    y, x, core = me // 4, lax.rem(me // 2, 2), lax.rem(me, 2)
    return [lax.rem(y + dy, 2) * 4 + lax.rem(x + dx, 2) * 2 + lax.rem(core + dc, 2) for dy, dx, dc in OFFSETS]


def stream_kernel(axis, rows, t_ref, x_hbm, w_hbm, b_hbm, cand_hbm, emb_hbm, z_ref, norm_ref, candz_ref,
                  ebuf, et_ref, x_ref, w_ref, b_ref, cand_ref, a_ref, m_ref, s_ref, q_ref, q_recv, st_ref, st_recv,
                  ecopy_sem, in_sem, q_sem, st_sem):
    width = x_ref.shape[1]
    chunks = rows // CHUNK
    inputs = [pltpu.make_async_copy(src, dst, in_sem.at[n]) for n, (src, dst) in enumerate(
        [(x_hbm, x_ref), (w_hbm, w_ref), (b_hbm, b_ref), (cand_hbm, cand_ref)])]
    for copy in inputs:
        copy.start()

    def fetch(i, slot):
        return pltpu.make_async_copy(emb_hbm.at[pl.ds(i * CHUNK, CHUNK), :], ebuf.at[slot], ecopy_sem.at[slot])

    for i in range(SLOTS):
        fetch(i, i).start()

    me = lax.axis_index(axis)
    peers = peers_of(me)
    barrier = pltpu.get_barrier_semaphore()
    for peer in peers:
        pl.semaphore_signal(barrier, inc=1, device_id=(peer,), device_id_type=MESH)

    for copy in inputs:
        copy.wait()
    x = x_ref[...].astype(jnp.float32)
    centered = x - jnp.mean(x, axis=-1, keepdims=True)
    var = jnp.mean(centered * centered, axis=-1, keepdims=True)
    scaled = centered * lax.rsqrt(var + 1e-5)
    gain, bias = w_ref[...].astype(jnp.float32), b_ref[...].astype(jnp.float32)
    for k in range(width // LANES):
        part = scaled[:, k * LANES:(k + 1) * LANES] * gain[k:k + 1, :] + bias[k:k + 1, :]
        a_ref[:, k * LANES:(k + 1) * LANES] = part.astype(jnp.bfloat16)
    m_ref[...] = jnp.full(m_ref.shape, -jnp.inf, jnp.float32)
    s_ref[...] = jnp.zeros(s_ref.shape, jnp.float32)
    q_ref[...] = jnp.zeros(q_ref.shape, jnp.float32)
    temp = t_ref[0]

    def logits(i, slot):
        for n, (first, size, flip) in enumerate(DOTS):
            tile = ebuf[slot, first:first + size, :]
            if flip:
                et_ref[n, :, :size] = tile.T
                z = jnp.dot(a_ref[...], et_ref[n, :, :size], preferred_element_type=jnp.float32)
            else:
                z = lax.dot_general(tile, a_ref[...], (((1,), (1,)), ((), ())), preferred_element_type=jnp.float32).T
            z_ref[:, pl.ds(pl.multiple_of(i * CHUNK + first, LANES), size)] = z / temp

    def tiles_of(i):
        return [z_ref[:, pl.ds(pl.multiple_of(i * CHUNK + t, LANES), LANES)] for t in range(0, CHUNK, LANES)]

    def candidates(i):
        cand = cand_ref[...] - me * rows - i * CHUNK
        lane, group = jnp.bitwise_and(cand, LANES - 1), jnp.right_shift(cand, 7)
        q = q_ref[...]
        for k, z in enumerate(tiles_of(i)):
            q = jnp.where(group == k, jnp.take_along_axis(z, lane, axis=1, mode="promise_in_bounds"), q)
        q_ref[...] = q

    def statistics(i):
        tiles = tiles_of(i)
        old = m_ref[...]
        new = functools.reduce(jnp.maximum, tiles, old)
        total = s_ref[...] * jnp.exp(old - new)
        for z in tiles:
            total = total + jnp.exp(z - new)
        m_ref[...] = new
        s_ref[...] = total

    fetch(0, 0).wait()
    logits(0, 0)

    @pl.loop(1, chunks)
    def _(i):
        @pl.when(i + SLOTS - 1 < chunks)
        def _():
            fetch(i + SLOTS - 1, lax.rem(i + SLOTS - 1, SLOTS)).start()

        fetch(i, lax.rem(i, SLOTS)).wait()
        statistics(i - 1)
        candidates(i - 1)
        logits(i, lax.rem(i, SLOTS))

    candidates(chunks - 1)
    pl.semaphore_wait(barrier, len(peers))

    def sends(src, dst, sems):
        return [pltpu.make_async_remote_copy(
            src_ref=src, dst_ref=dst.at[k], send_sem=sems.at[0, k], recv_sem=sems.at[1, k],
            device_id=(peer,), device_id_type=MESH) for k, peer in enumerate(peers)]

    q_copies = sends(q_ref, q_recv, q_sem)
    for copy in q_copies:
        copy.start()
    statistics(chunks - 1)
    m = m_ref[...]
    row_max = jnp.max(m, axis=1, keepdims=True)
    local = row_max + jnp.log(jnp.sum(s_ref[...] * jnp.exp(m - row_max), axis=1, keepdims=True))
    diagonal = lax.broadcasted_iota(jnp.int32, m.shape, 0) == lax.broadcasted_iota(jnp.int32, m.shape, 1)
    mine = jnp.sum(jnp.where(diagonal, local, 0.0), axis=0, keepdims=True)
    st_ref[...] = mine
    st_copies = sends(st_ref, st_recv, st_sem)
    for copy in st_copies:
        copy.start()
    for copy in st_copies:
        copy.wait()
    parts = [mine] + [st_recv[k] for k in range(len(peers))]
    top = functools.reduce(jnp.maximum, parts)
    norm = top + jnp.log(functools.reduce(jnp.add, [jnp.exp(p - top) for p in parts]))
    norm = jnp.sum(jnp.where(diagonal, norm, 0.0), axis=1, keepdims=True)
    norm_ref[...] = jnp.broadcast_to(norm, norm_ref.shape)
    for copy in q_copies:
        copy.wait()
    candz_ref[...] = functools.reduce(jnp.add, [q_recv[k] for k in range(len(peers))], q_ref[...])


def finish_kernel(z_ref, norm_ref, candz_ref, lp_hbm, q_hbm, buf, q_ref, sem):
    norm = norm_ref[...]
    q_ref[...] = candz_ref[...] - norm
    copies, start = [pltpu.make_async_copy(q_ref, q_hbm, sem.at[len(PIECES)])], 0
    for n, size in enumerate(PIECES):
        for c in range(start, start + size, LANES):
            buf[:, c:c + LANES] = z_ref[:, c:c + LANES] - norm
        copies.append(pltpu.make_async_copy(buf.at[:, pl.ds(start, size)], lp_hbm.at[:, pl.ds(start, size)], sem.at[n]))
        copies[-1].start()
        start += size
        if n == 0:
            copies[0].start()
    for copy in copies:
        copy.wait()


def solution(mesh):
    axis = mesh.axis_names[0]

    def per_device(hidden, ln_weight, ln_bias, emb, temperature, cand_ids):
        batch, width = hidden.shape
        rows = emb.shape[0]
        vmem = pl.BlockSpec(memory_space=pltpu.VMEM)
        hbm = pl.BlockSpec(memory_space=pl.ANY)
        f32, bf16 = jnp.float32, jnp.bfloat16
        dma = pltpu.SemaphoreType.DMA
        block = (width // LANES, LANES)
        small = [hidden, ln_weight.reshape(block), ln_bias.reshape(block), cand_ids]
        small = [pltpu.with_memory_space_constraint(v, pltpu.HBM) for v in small]
        z, norm, candz = pl.pallas_call(
            functools.partial(stream_kernel, axis, rows),
            out_shape=(pltpu.VMEM((batch, rows), f32), pltpu.VMEM((batch, LANES), f32),
                       pltpu.VMEM((batch, LANES), f32)),
            in_specs=[pl.BlockSpec(memory_space=pltpu.SMEM)] + [hbm] * 5,
            out_specs=(vmem, vmem, vmem),
            scratch_shapes=[
                pltpu.VMEM((SLOTS, CHUNK, width), bf16),
                pltpu.VMEM((len(DOTS), width, 256), bf16),
                pltpu.VMEM((batch, width), bf16),
                pltpu.VMEM(block, bf16),
                pltpu.VMEM(block, bf16),
                pltpu.VMEM((batch, LANES), jnp.int32),
                pltpu.VMEM((batch, width), bf16),
                pltpu.VMEM((batch, LANES), f32),
                pltpu.VMEM((batch, LANES), f32),
                pltpu.VMEM((batch, LANES), f32),
                pltpu.VMEM((len(OFFSETS), batch, LANES), f32),
                pltpu.VMEM((1, LANES), f32),
                pltpu.VMEM((len(OFFSETS), 1, LANES), f32),
                dma((SLOTS,)), dma((4,)), dma((2, 7)), dma((2, 7)),
            ],
            compiler_params=pltpu.CompilerParams(
                collective_id=0, has_side_effects=True, vmem_limit_bytes=48 * 1024 * 1024),
        )(temperature.reshape(1), *small, emb)
        return pl.pallas_call(
            finish_kernel,
            out_shape=(jax.ShapeDtypeStruct((batch, rows), f32), jax.ShapeDtypeStruct((batch, LANES), f32)),
            in_specs=[vmem, vmem, vmem],
            out_specs=(hbm, hbm),
            scratch_shapes=[pltpu.VMEM((batch, rows), f32), pltpu.VMEM((batch, LANES), f32),
                            dma((len(PIECES) + 1,))],
            compiler_params=pltpu.CompilerParams(vmem_limit_bytes=16 * 1024 * 1024),
        )(z, norm, candz)

    return jax.shard_map(
        per_device,
        mesh=mesh,
        in_specs=(P(), P(), P(), P(axis, None), P(), P()),
        out_specs=(P(None, axis), P()),
        check_vma=False,
    )
```

```python
import functools

import jax
import jax.numpy as jnp
from jax import lax
from jax.experimental import pallas as pl
from jax.experimental.pallas import tpu as pltpu
from jax.sharding import PartitionSpec as P

LANES = 128
CHUNK = 896
SLOTS = 5
DOTS = ((0, 128, False), (128, 256, False), (384, 256, True), (640, 256, True))
PIECES = (896, 1792, 3584, 6272, 6272, 6272, 6272)
DEVICES = 8
MESH = pl.DeviceIdType.MESH


def peers_of(me):
    return [k + (k + DEVICES - me) // DEVICES for k in range(DEVICES - 1)]


def stream_kernel(axis, rows, t_ref, x_hbm, w_hbm, b_hbm, cand_hbm, emb_hbm, z_ref, norm_ref, candz_ref,
                  ebuf, et_ref, x_ref, w_ref, b_ref, cand_ref, a_ref, m_ref, s_ref, q_ref, q_recv, st_ref, st_recv,
                  ecopy_sem, in_sem, q_sem, st_sem):
    width = x_ref.shape[1]
    chunks = rows // CHUNK
    inputs = [pltpu.make_async_copy(src, dst, in_sem.at[n]) for n, (src, dst) in enumerate(
        [(x_hbm, x_ref), (w_hbm, w_ref), (b_hbm, b_ref), (cand_hbm, cand_ref)])]
    for copy in inputs:
        copy.start()

    def fetch(i, slot):
        return pltpu.make_async_copy(emb_hbm.at[pl.ds(i * CHUNK, CHUNK), :], ebuf.at[slot], ecopy_sem.at[slot])

    for i in range(SLOTS):
        fetch(i, i).start()

    me = lax.axis_index(axis)
    peers = peers_of(me)
    barrier = pltpu.get_barrier_semaphore()
    for peer in peers:
        pl.semaphore_signal(barrier, inc=1, device_id=(peer,), device_id_type=MESH)

    for copy in inputs:
        copy.wait()
    x = x_ref[...].astype(jnp.float32)
    centered = x - jnp.mean(x, axis=-1, keepdims=True)
    var = jnp.mean(centered * centered, axis=-1, keepdims=True)
    scaled = centered * lax.rsqrt(var + 1e-5)
    gain, bias = w_ref[...].astype(jnp.float32), b_ref[...].astype(jnp.float32)
    for k in range(width // LANES):
        part = scaled[:, k * LANES:(k + 1) * LANES] * gain[k:k + 1, :] + bias[k:k + 1, :]
        a_ref[:, k * LANES:(k + 1) * LANES] = part.astype(jnp.bfloat16)
    m_ref[...] = jnp.full(m_ref.shape, -jnp.inf, jnp.float32)
    s_ref[...] = jnp.zeros(s_ref.shape, jnp.float32)
    q_ref[...] = jnp.zeros(q_ref.shape, jnp.float32)
    temp = t_ref[0]

    def logits(i, slot):
        for n, (first, size, flip) in enumerate(DOTS):
            tile = ebuf[slot, first:first + size, :]
            if flip:
                et_ref[n, :, :size] = tile.T
                z = jnp.dot(a_ref[...], et_ref[n, :, :size], preferred_element_type=jnp.float32)
            else:
                z = lax.dot_general(tile, a_ref[...], (((1,), (1,)), ((), ())), preferred_element_type=jnp.float32).T
            z_ref[:, pl.ds(pl.multiple_of(i * CHUNK + first, LANES), size)] = z / temp

    def tiles_of(i):
        return [z_ref[:, pl.ds(pl.multiple_of(i * CHUNK + t, LANES), LANES)] for t in range(0, CHUNK, LANES)]

    def candidates(i):
        cand = cand_ref[...] - me * rows - i * CHUNK
        lane, group = jnp.bitwise_and(cand, LANES - 1), jnp.right_shift(cand, 7)
        q = q_ref[...]
        for k, z in enumerate(tiles_of(i)):
            q = jnp.where(group == k, jnp.take_along_axis(z, lane, axis=1, mode="promise_in_bounds"), q)
        q_ref[...] = q

    def statistics(i):
        tiles = tiles_of(i)
        old = m_ref[...]
        new = functools.reduce(jnp.maximum, tiles, old)
        total = s_ref[...] * jnp.exp(old - new)
        for z in tiles:
            total = total + jnp.exp(z - new)
        m_ref[...] = new
        s_ref[...] = total

    fetch(0, 0).wait()
    logits(0, 0)

    @pl.loop(1, chunks)
    def _(i):
        @pl.when(i + SLOTS - 1 < chunks)
        def _():
            fetch(i + SLOTS - 1, lax.rem(i + SLOTS - 1, SLOTS)).start()

        fetch(i, lax.rem(i, SLOTS)).wait()
        statistics(i - 1)
        candidates(i - 1)
        logits(i, lax.rem(i, SLOTS))

    candidates(chunks - 1)
    statistics(chunks - 1)
    m = m_ref[...]
    row_max = jnp.max(m, axis=1, keepdims=True)
    local = row_max + jnp.log(jnp.sum(s_ref[...] * jnp.exp(m - row_max), axis=1, keepdims=True))
    diagonal = lax.broadcasted_iota(jnp.int32, m.shape, 0) == lax.broadcasted_iota(jnp.int32, m.shape, 1)
    mine = jnp.sum(jnp.where(diagonal, local, 0.0), axis=0, keepdims=True)
    st_ref[...] = mine

    pl.semaphore_wait(barrier, len(peers))

    def send(src, dst, sems, peer):
        slot = me - (me - peer + DEVICES - 1) // DEVICES
        pltpu.make_async_remote_copy(
            src_ref=src, dst_ref=dst.at[slot], send_sem=sems.at[0], recv_sem=sems.at[1],
            device_id=(peer,), device_id_type=MESH).start()

    def all_of(buf, sems):
        return pltpu.make_async_remote_copy(
            src_ref=buf, dst_ref=buf, send_sem=sems.at[0], recv_sem=sems.at[1],
            device_id=(peers[0],), device_id_type=MESH)

    for peer in peers[:2]:
        send(st_ref, st_recv, st_sem, peer)
    for peer in peers[:2]:
        send(q_ref, q_recv, q_sem, peer)
    for peer in peers[2:]:
        send(st_ref, st_recv, st_sem, peer)
    for peer in peers[2:]:
        send(q_ref, q_recv, q_sem, peer)
    all_of(st_recv, st_sem).wait_recv()
    parts = [mine] + [st_recv[k] for k in range(len(peers))]
    top = functools.reduce(jnp.maximum, parts)
    norm = top + jnp.log(functools.reduce(jnp.add, [jnp.exp(p - top) for p in parts]))
    norm = jnp.sum(jnp.where(diagonal, norm, 0.0), axis=1, keepdims=True)
    norm_ref[...] = jnp.broadcast_to(norm, norm_ref.shape)
    all_of(q_recv, q_sem).wait_recv()
    candz_ref[...] = functools.reduce(jnp.add, [q_recv[k] for k in range(len(peers))], q_ref[...])
    all_of(st_recv, st_sem).wait_send()
    all_of(q_recv, q_sem).wait_send()


def finish_kernel(z_ref, norm_ref, candz_ref, lp_hbm, q_hbm, buf, q_ref, sem):
    norm = norm_ref[...]
    q_ref[...] = candz_ref[...] - norm
    copies, start = [pltpu.make_async_copy(q_ref, q_hbm, sem.at[len(PIECES)])], 0
    for n, size in enumerate(PIECES):
        for c in range(start, start + size, LANES):
            buf[:, c:c + LANES] = z_ref[:, c:c + LANES] - norm
        copies.append(pltpu.make_async_copy(buf.at[:, pl.ds(start, size)], lp_hbm.at[:, pl.ds(start, size)], sem.at[n]))
        copies[-1].start()
        start += size
        if n == 0:
            copies[0].start()
    for copy in copies:
        copy.wait()


def solution(mesh):
    axis = mesh.axis_names[0]

    def per_device(hidden, ln_weight, ln_bias, emb, temperature, cand_ids):
        batch, width = hidden.shape
        rows = emb.shape[0]
        vmem = pl.BlockSpec(memory_space=pltpu.VMEM)
        hbm = pl.BlockSpec(memory_space=pl.ANY)
        f32, bf16 = jnp.float32, jnp.bfloat16
        dma = pltpu.SemaphoreType.DMA
        block = (width // LANES, LANES)
        small = [hidden, ln_weight.reshape(block), ln_bias.reshape(block), cand_ids]
        small = [pltpu.with_memory_space_constraint(v, pltpu.HBM) for v in small]
        z, norm, candz = pl.pallas_call(
            functools.partial(stream_kernel, axis, rows),
            out_shape=(pltpu.VMEM((batch, rows), f32), pltpu.VMEM((batch, LANES), f32),
                       pltpu.VMEM((batch, LANES), f32)),
            in_specs=[pl.BlockSpec(memory_space=pltpu.SMEM)] + [hbm] * 5,
            out_specs=(vmem, vmem, vmem),
            scratch_shapes=[
                pltpu.VMEM((SLOTS, CHUNK, width), bf16),
                pltpu.VMEM((len(DOTS), width, 256), bf16),
                pltpu.VMEM((batch, width), bf16),
                pltpu.VMEM(block, bf16),
                pltpu.VMEM(block, bf16),
                pltpu.VMEM((batch, LANES), jnp.int32),
                pltpu.VMEM((batch, width), bf16),
                pltpu.VMEM((batch, LANES), f32),
                pltpu.VMEM((batch, LANES), f32),
                pltpu.VMEM((batch, LANES), f32),
                pltpu.VMEM((DEVICES - 1, batch, LANES), f32),
                pltpu.VMEM((1, LANES), f32),
                pltpu.VMEM((DEVICES - 1, 1, LANES), f32),
                dma((SLOTS,)), dma((4,)), dma((2,)), dma((2,)),
            ],
            compiler_params=pltpu.CompilerParams(
                collective_id=0, has_side_effects=True, vmem_limit_bytes=48 * 1024 * 1024),
        )(temperature.reshape(1), *small, emb)
        return pl.pallas_call(
            finish_kernel,
            out_shape=(jax.ShapeDtypeStruct((batch, rows), f32), jax.ShapeDtypeStruct((batch, LANES), f32)),
            in_specs=[vmem, vmem, vmem],
            out_specs=(hbm, hbm),
            scratch_shapes=[pltpu.VMEM((batch, rows), f32), pltpu.VMEM((batch, LANES), f32),
                            dma((len(PIECES) + 1,))],
            compiler_params=pltpu.CompilerParams(vmem_limit_bytes=16 * 1024 * 1024),
        )(z, norm, candz)

    return jax.shard_map(
        per_device,
        mesh=mesh,
        in_specs=(P(), P(), P(), P(axis, None), P(), P()),
        out_specs=(P(None, axis), P()),
        check_vma=False,
    )
```

```python
import functools

import jax
import jax.numpy as jnp
from jax import lax
from jax.experimental import pallas as pl
from jax.experimental.pallas import tpu as pltpu
from jax.sharding import PartitionSpec as P

LANES = 128
CHUNK = 896
SLOTS = 5
DOTS = ((0, 128, False), (128, 256, False), (384, 256, True), (640, 256, True))
PIECES = (896, 1792, 3584, 6272, 6272, 6272, 6272)
DEVICES = 8
MESH = pl.DeviceIdType.MESH


def peers_of(me):
    return [k + (k + DEVICES - me) // DEVICES for k in range(DEVICES - 1)]


def stream_kernel(axis, rows, x_hbm, w_hbm, b_hbm, cand_hbm, t_hbm, emb_hbm, z_ref, norm_ref, candz_ref,
                  ebuf, et_ref, x_ref, w_ref, b_ref, cand_ref, t_ref, a_ref, m_ref, s_ref, q_ref, q_recv, st_ref, st_recv,
                  ecopy_sem, in_sem, q_sem, st_sem):
    width = x_ref.shape[1]
    chunks = rows // CHUNK
    inputs = [pltpu.make_async_copy(src, dst, in_sem.at[n]) for n, (src, dst) in enumerate(
        [(x_hbm, x_ref), (w_hbm, w_ref), (b_hbm, b_ref), (cand_hbm, cand_ref), (t_hbm, t_ref)])]
    for copy in inputs:
        copy.start()

    def fetch(i, slot):
        return pltpu.make_async_copy(emb_hbm.at[pl.ds(i * CHUNK, CHUNK), :], ebuf.at[slot], ecopy_sem.at[slot])

    for i in range(SLOTS):
        fetch(i, i).start()

    me = lax.axis_index(axis)
    peers = peers_of(me)
    barrier = pltpu.get_barrier_semaphore()
    for peer in peers:
        pl.semaphore_signal(barrier, inc=1, device_id=(peer,), device_id_type=MESH)

    for copy in inputs:
        copy.wait()
    x = x_ref[...].astype(jnp.float32)
    centered = x - jnp.mean(x, axis=-1, keepdims=True)
    var = jnp.mean(centered * centered, axis=-1, keepdims=True)
    scaled = centered * lax.rsqrt(var + 1e-5)
    gain, bias = w_ref[...].astype(jnp.float32), b_ref[...].astype(jnp.float32)
    for k in range(width // LANES):
        part = scaled[:, k * LANES:(k + 1) * LANES] * gain[k:k + 1, :] + bias[k:k + 1, :]
        a_ref[:, k * LANES:(k + 1) * LANES] = part.astype(jnp.bfloat16)
    m_ref[...] = jnp.full(m_ref.shape, -jnp.inf, jnp.float32)
    s_ref[...] = jnp.zeros(s_ref.shape, jnp.float32)
    q_ref[...] = jnp.zeros(q_ref.shape, jnp.float32)
    temp = t_ref[0]

    def logits(i, slot):
        for n, (first, size, flip) in enumerate(DOTS):
            tile = ebuf[slot, first:first + size, :]
            if flip:
                et_ref[n, :, :size] = tile.T
                z = jnp.dot(a_ref[...], et_ref[n, :, :size], preferred_element_type=jnp.float32)
            else:
                z = lax.dot_general(tile, a_ref[...], (((1,), (1,)), ((), ())), preferred_element_type=jnp.float32).T
            z_ref[:, pl.ds(pl.multiple_of(i * CHUNK + first, LANES), size)] = z / temp

    def tiles_of(i):
        return [z_ref[:, pl.ds(pl.multiple_of(i * CHUNK + t, LANES), LANES)] for t in range(0, CHUNK, LANES)]

    def candidates(i):
        cand = cand_ref[...] - me * rows - i * CHUNK
        lane, group = jnp.bitwise_and(cand, LANES - 1), jnp.right_shift(cand, 7)
        q = q_ref[...]
        for k, z in enumerate(tiles_of(i)):
            q = jnp.where(group == k, jnp.take_along_axis(z, lane, axis=1, mode="promise_in_bounds"), q)
        q_ref[...] = q

    def statistics(i):
        tiles = tiles_of(i)
        old = m_ref[...]
        new = functools.reduce(jnp.maximum, tiles, old)
        total = s_ref[...] * jnp.exp(old - new)
        for z in tiles:
            total = total + jnp.exp(z - new)
        m_ref[...] = new
        s_ref[...] = total

    fetch(0, 0).wait()
    logits(0, 0)

    @pl.loop(1, chunks)
    def _(i):
        @pl.when(i + SLOTS - 1 < chunks)
        def _():
            fetch(i + SLOTS - 1, lax.rem(i + SLOTS - 1, SLOTS)).start()

        fetch(i, lax.rem(i, SLOTS)).wait()
        statistics(i - 1)
        candidates(i - 1)
        logits(i, lax.rem(i, SLOTS))

    candidates(chunks - 1)
    statistics(chunks - 1)
    m = m_ref[...]
    row_max = jnp.max(m, axis=1, keepdims=True)
    local = row_max + jnp.log(jnp.sum(s_ref[...] * jnp.exp(m - row_max), axis=1, keepdims=True))
    diagonal = lax.broadcasted_iota(jnp.int32, m.shape, 0) == lax.broadcasted_iota(jnp.int32, m.shape, 1)
    mine = jnp.sum(jnp.where(diagonal, local, 0.0), axis=0, keepdims=True)
    st_ref[...] = mine

    pl.semaphore_wait(barrier, len(peers))

    def send(src, dst, sems, peer):
        slot = me - (me - peer + DEVICES - 1) // DEVICES
        pltpu.make_async_remote_copy(
            src_ref=src, dst_ref=dst.at[slot], send_sem=sems.at[0], recv_sem=sems.at[1],
            device_id=(peer,), device_id_type=MESH).start()

    def all_of(buf, sems):
        return pltpu.make_async_remote_copy(
            src_ref=buf, dst_ref=buf, send_sem=sems.at[0], recv_sem=sems.at[1],
            device_id=(peers[0],), device_id_type=MESH)

    for peer in peers[:2]:
        send(st_ref, st_recv, st_sem, peer)
    for peer in peers[:2]:
        send(q_ref, q_recv, q_sem, peer)
    for peer in peers[2:]:
        send(st_ref, st_recv, st_sem, peer)
    for peer in peers[2:]:
        send(q_ref, q_recv, q_sem, peer)
    all_of(st_recv, st_sem).wait_recv()
    parts = [mine] + [st_recv[k] for k in range(len(peers))]
    top = functools.reduce(jnp.maximum, parts)
    norm = top + jnp.log(functools.reduce(jnp.add, [jnp.exp(p - top) for p in parts]))
    norm = jnp.sum(jnp.where(diagonal, norm, 0.0), axis=1, keepdims=True)
    norm_ref[...] = jnp.broadcast_to(norm, norm_ref.shape)
    all_of(q_recv, q_sem).wait_recv()
    candz_ref[...] = functools.reduce(jnp.add, [q_recv[k] for k in range(len(peers))], q_ref[...])
    all_of(st_recv, st_sem).wait_send()
    all_of(q_recv, q_sem).wait_send()


def finish_kernel(z_ref, norm_ref, candz_ref, lp_hbm, q_hbm, buf, q_ref, sem):
    norm = norm_ref[...]
    q_ref[...] = candz_ref[...] - norm
    copies, start = [pltpu.make_async_copy(q_ref, q_hbm, sem.at[len(PIECES)])], 0
    for n, size in enumerate(PIECES):
        for c in range(start, start + size, LANES):
            buf[:, c:c + LANES] = z_ref[:, c:c + LANES] - norm
        copies.append(pltpu.make_async_copy(buf.at[:, pl.ds(start, size)], lp_hbm.at[:, pl.ds(start, size)], sem.at[n]))
        copies[-1].start()
        start += size
        if n == 0:
            copies[0].start()
    for copy in copies:
        copy.wait()


def solution(mesh):
    axis = mesh.axis_names[0]

    def per_device(hidden, ln_weight, ln_bias, emb, temperature, cand_ids):
        batch, width = hidden.shape
        rows = emb.shape[0]
        vmem = pl.BlockSpec(memory_space=pltpu.VMEM)
        hbm = pl.BlockSpec(memory_space=pl.ANY)
        f32, bf16 = jnp.float32, jnp.bfloat16
        dma = pltpu.SemaphoreType.DMA
        block = (width // LANES, LANES)
        small = [hidden, ln_weight.reshape(block), ln_bias.reshape(block), cand_ids, temperature.reshape(1)]
        small = [pltpu.with_memory_space_constraint(v, pltpu.HBM) for v in small[:4]] + small[4:]
        z, norm, candz = pl.pallas_call(
            functools.partial(stream_kernel, axis, rows),
            out_shape=(pltpu.VMEM((batch, rows), f32), pltpu.VMEM((batch, LANES), f32),
                       pltpu.VMEM((batch, LANES), f32)),
            in_specs=[hbm] * 6,
            out_specs=(vmem, vmem, vmem),
            scratch_shapes=[
                pltpu.VMEM((SLOTS, CHUNK, width), bf16),
                pltpu.VMEM((len(DOTS), width, 256), bf16),
                pltpu.VMEM((batch, width), bf16),
                pltpu.VMEM(block, bf16),
                pltpu.VMEM(block, bf16),
                pltpu.VMEM((batch, LANES), jnp.int32),
                pltpu.SMEM((1,), f32),
                pltpu.VMEM((batch, width), bf16),
                pltpu.VMEM((batch, LANES), f32),
                pltpu.VMEM((batch, LANES), f32),
                pltpu.VMEM((batch, LANES), f32),
                pltpu.VMEM((DEVICES - 1, batch, LANES), f32),
                pltpu.VMEM((1, LANES), f32),
                pltpu.VMEM((DEVICES - 1, 1, LANES), f32),
                dma((SLOTS,)), dma((5,)), dma((2,)), dma((2,)),
            ],
            compiler_params=pltpu.CompilerParams(
                collective_id=0, has_side_effects=True, vmem_limit_bytes=48 * 1024 * 1024),
        )(*small, emb)
        return pl.pallas_call(
            finish_kernel,
            out_shape=(jax.ShapeDtypeStruct((batch, rows), f32), jax.ShapeDtypeStruct((batch, LANES), f32)),
            in_specs=[vmem, vmem, vmem],
            out_specs=(hbm, hbm),
            scratch_shapes=[pltpu.VMEM((batch, rows), f32), pltpu.VMEM((batch, LANES), f32),
                            dma((len(PIECES) + 1,))],
            compiler_params=pltpu.CompilerParams(vmem_limit_bytes=16 * 1024 * 1024),
        )(z, norm, candz)

    return jax.shard_map(
        per_device,
        mesh=mesh,
        in_specs=(P(), P(), P(), P(axis, None), P(), P()),
        out_specs=(P(None, axis), P()),
        check_vma=False,
    )
```

```python
import functools

import jax
import jax.numpy as jnp
from jax import lax
from jax.experimental import pallas as pl
from jax.experimental.pallas import tpu as pltpu
from jax.sharding import PartitionSpec as P

LANES = 128
CHUNK = 896
SLOTS = 5
DOTS = ((0, 128, False), (128, 256, False), (384, 256, True), (640, 256, True))
PIECES = (896, 1792, 3584, 6272, 6272, 6272, 6272)
DEVICES = 8
MESH = pl.DeviceIdType.MESH


def peers_of(me):
    return [k + (k + DEVICES - me) // DEVICES for k in range(DEVICES - 1)]


def stream_kernel(axis, rows, x_hbm, w_hbm, b_hbm, cand_hbm, t_hbm, emb_hbm, z_ref, norm_ref, candz_ref,
                  ebuf, et_ref, x_ref, w_ref, b_ref, cand_ref, t_ref, a_ref, m_ref, s_ref, q_ref, q_recv, st_ref, st_recv,
                  ecopy_sem, in_sem, q_sem, st_sem):
    width = x_ref.shape[1]
    chunks = rows // CHUNK
    inputs = [pltpu.make_async_copy(src, dst, in_sem.at[n]) for n, (src, dst) in enumerate(
        [(x_hbm, x_ref), (w_hbm, w_ref), (b_hbm, b_ref), (cand_hbm, cand_ref), (t_hbm, t_ref)])]
    for copy in inputs:
        copy.start()

    def fetch(i, slot):
        return pltpu.make_async_copy(emb_hbm.at[pl.ds(i * CHUNK, CHUNK), :], ebuf.at[slot], ecopy_sem.at[slot])

    for i in range(SLOTS):
        fetch(i, i).start()

    me = lax.axis_index(axis)
    peers = peers_of(me)
    barrier = pltpu.get_barrier_semaphore()
    for peer in peers:
        pl.semaphore_signal(barrier, inc=1, device_id=(peer,), device_id_type=MESH)

    for copy in inputs:
        copy.wait()
    x = x_ref[...].astype(jnp.float32)
    centered = x - jnp.mean(x, axis=-1, keepdims=True)
    var = jnp.mean(centered * centered, axis=-1, keepdims=True)
    scaled = centered * lax.rsqrt(var + 1e-5)
    gain, bias = w_ref[...].astype(jnp.float32), b_ref[...].astype(jnp.float32)
    for k in range(width // LANES):
        part = scaled[:, k * LANES:(k + 1) * LANES] * gain[k:k + 1, :] + bias[k:k + 1, :]
        a_ref[:, k * LANES:(k + 1) * LANES] = part.astype(jnp.bfloat16)
    m_ref[...] = jnp.full(m_ref.shape, -jnp.inf, jnp.float32)
    s_ref[...] = jnp.zeros(s_ref.shape, jnp.float32)
    q_ref[...] = jnp.zeros(q_ref.shape, jnp.float32)
    temp = t_ref[0]

    def logits(i, slot):
        for n, (first, size, flip) in enumerate(DOTS):
            tile = ebuf[slot, first:first + size, :]
            if flip:
                et_ref[n, :, :size] = tile.T
                z = jnp.dot(a_ref[...], et_ref[n, :, :size], preferred_element_type=jnp.float32)
            else:
                z = lax.dot_general(tile, a_ref[...], (((1,), (1,)), ((), ())), preferred_element_type=jnp.float32).T
            z_ref[:, pl.ds(pl.multiple_of(i * CHUNK + first, LANES), size)] = z / temp

    def tiles_of(i):
        return [z_ref[:, pl.ds(pl.multiple_of(i * CHUNK + t, LANES), LANES)] for t in range(0, CHUNK, LANES)]

    def candidates(i):
        cand = cand_ref[...] - me * rows - i * CHUNK
        lane, group = jnp.bitwise_and(cand, LANES - 1), jnp.right_shift(cand, 7)
        q = q_ref[...]
        for k, z in enumerate(tiles_of(i)):
            q = jnp.where(group == k, jnp.take_along_axis(z, lane, axis=1, mode="promise_in_bounds"), q)
        q_ref[...] = q

    def statistics(i):
        tiles = tiles_of(i)
        old = m_ref[...]
        new = functools.reduce(jnp.maximum, tiles, old)
        total = s_ref[...] * jnp.exp(old - new)
        for z in tiles:
            total = total + jnp.exp(z - new)
        m_ref[...] = new
        s_ref[...] = total

    fetch(0, 0).wait()
    logits(0, 0)

    @pl.loop(1, chunks - 1)
    def _(i):
        @pl.when(i + SLOTS - 1 < chunks)
        def _():
            fetch(i + SLOTS - 1, lax.rem(i + SLOTS - 1, SLOTS)).start()

        fetch(i, lax.rem(i, SLOTS)).wait()
        statistics(i - 1)
        candidates(i - 1)
        logits(i, lax.rem(i, SLOTS))

    statistics(chunks - 2)
    candidates(chunks - 2)
    pl.semaphore_wait(barrier, len(peers))
    fetch(chunks - 1, (chunks - 1) % SLOTS).wait()
    logits(chunks - 1, (chunks - 1) % SLOTS)
    statistics(chunks - 1)
    candidates(chunks - 1)
    m = m_ref[...]
    row_max = jnp.max(m, axis=1, keepdims=True)
    local = row_max + jnp.log(jnp.sum(s_ref[...] * jnp.exp(m - row_max), axis=1, keepdims=True))
    diagonal = lax.broadcasted_iota(jnp.int32, m.shape, 0) == lax.broadcasted_iota(jnp.int32, m.shape, 1)
    mine = jnp.sum(jnp.where(diagonal, local, 0.0), axis=0, keepdims=True)
    st_ref[...] = mine

    def send(src, dst, sems, peer):
        slot = me - (me - peer + DEVICES - 1) // DEVICES
        pltpu.make_async_remote_copy(
            src_ref=src, dst_ref=dst.at[slot], send_sem=sems.at[0], recv_sem=sems.at[1],
            device_id=(peer,), device_id_type=MESH).start()

    def all_of(buf, sems):
        return pltpu.make_async_remote_copy(
            src_ref=buf, dst_ref=buf, send_sem=sems.at[0], recv_sem=sems.at[1],
            device_id=(peers[0],), device_id_type=MESH)

    for peer in peers[:2]:
        send(st_ref, st_recv, st_sem, peer)
    for peer in peers[:2]:
        send(q_ref, q_recv, q_sem, peer)
    for peer in peers[2:]:
        send(st_ref, st_recv, st_sem, peer)
    for peer in peers[2:]:
        send(q_ref, q_recv, q_sem, peer)
    all_of(st_recv, st_sem).wait_recv()
    parts = [mine] + [st_recv[k] for k in range(len(peers))]
    top = functools.reduce(jnp.maximum, parts)
    norm = top + jnp.log(functools.reduce(jnp.add, [jnp.exp(p - top) for p in parts]))
    norm = jnp.sum(jnp.where(diagonal, norm, 0.0), axis=1, keepdims=True)
    norm_ref[...] = jnp.broadcast_to(norm, norm_ref.shape)
    all_of(q_recv, q_sem).wait_recv()
    candz_ref[...] = functools.reduce(jnp.add, [q_recv[k] for k in range(len(peers))], q_ref[...])
    all_of(st_recv, st_sem).wait_send()
    all_of(q_recv, q_sem).wait_send()


def finish_kernel(z_ref, norm_ref, candz_ref, lp_hbm, q_hbm, buf, q_ref, sem):
    norm = norm_ref[...]
    q_ref[...] = candz_ref[...] - norm
    copies, start = [pltpu.make_async_copy(q_ref, q_hbm, sem.at[len(PIECES)])], 0
    for n, size in enumerate(PIECES):
        for c in range(start, start + size, LANES):
            buf[:, c:c + LANES] = z_ref[:, c:c + LANES] - norm
        copies.append(pltpu.make_async_copy(buf.at[:, pl.ds(start, size)], lp_hbm.at[:, pl.ds(start, size)], sem.at[n]))
        copies[-1].start()
        start += size
        if n == 0:
            copies[0].start()
    for copy in copies:
        copy.wait()


def solution(mesh):
    axis = mesh.axis_names[0]

    def per_device(hidden, ln_weight, ln_bias, emb, temperature, cand_ids):
        batch, width = hidden.shape
        rows = emb.shape[0]
        vmem = pl.BlockSpec(memory_space=pltpu.VMEM)
        hbm = pl.BlockSpec(memory_space=pl.ANY)
        f32, bf16 = jnp.float32, jnp.bfloat16
        dma = pltpu.SemaphoreType.DMA
        block = (width // LANES, LANES)
        small = [hidden, ln_weight.reshape(block), ln_bias.reshape(block), cand_ids, temperature.reshape(1)]
        small = [pltpu.with_memory_space_constraint(v, pltpu.HBM) for v in small[:4]] + small[4:]
        z, norm, candz = pl.pallas_call(
            functools.partial(stream_kernel, axis, rows),
            out_shape=(pltpu.VMEM((batch, rows), f32), pltpu.VMEM((batch, LANES), f32),
                       pltpu.VMEM((batch, LANES), f32)),
            in_specs=[hbm] * 6,
            out_specs=(vmem, vmem, vmem),
            scratch_shapes=[
                pltpu.VMEM((SLOTS, CHUNK, width), bf16),
                pltpu.VMEM((len(DOTS), width, 256), bf16),
                pltpu.VMEM((batch, width), bf16),
                pltpu.VMEM(block, bf16),
                pltpu.VMEM(block, bf16),
                pltpu.VMEM((batch, LANES), jnp.int32),
                pltpu.SMEM((1,), f32),
                pltpu.VMEM((batch, width), bf16),
                pltpu.VMEM((batch, LANES), f32),
                pltpu.VMEM((batch, LANES), f32),
                pltpu.VMEM((batch, LANES), f32),
                pltpu.VMEM((DEVICES - 1, batch, LANES), f32),
                pltpu.VMEM((1, LANES), f32),
                pltpu.VMEM((DEVICES - 1, 1, LANES), f32),
                dma((SLOTS,)), dma((5,)), dma((2,)), dma((2,)),
            ],
            compiler_params=pltpu.CompilerParams(
                collective_id=0, has_side_effects=True, vmem_limit_bytes=48 * 1024 * 1024),
        )(*small, emb)
        return pl.pallas_call(
            finish_kernel,
            out_shape=(jax.ShapeDtypeStruct((batch, rows), f32), jax.ShapeDtypeStruct((batch, LANES), f32)),
            in_specs=[vmem, vmem, vmem],
            out_specs=(hbm, hbm),
            scratch_shapes=[pltpu.VMEM((batch, rows), f32), pltpu.VMEM((batch, LANES), f32),
                            dma((len(PIECES) + 1,))],
            compiler_params=pltpu.CompilerParams(vmem_limit_bytes=16 * 1024 * 1024),
        )(z, norm, candz)

    return jax.shard_map(
        per_device,
        mesh=mesh,
        in_specs=(P(), P(), P(), P(axis, None), P(), P()),
        out_specs=(P(None, axis), P()),
        check_vma=False,
    )
```

```python
import functools

import jax
import jax.numpy as jnp
from jax import lax
from jax.experimental import pallas as pl
from jax.experimental.pallas import tpu as pltpu
from jax.sharding import PartitionSpec as P

LANES = 128
CHUNK = 896
GROUP = 2
SINGLES = 5
SLOTS = 4
DOTS = ((0, 128, False), (128, 256, False), (384, 256, True), (640, 256, True))
GROUP_DOTS = tuple((256 * n, 256, n >= 3) for n in range(7))
PIECES = (896, 1792, 3584, 6272, 6272, 6272, 6272)
DEVICES = 8
MESH = pl.DeviceIdType.MESH


def peers_of(me):
    return [k + (k + DEVICES - me) // DEVICES for k in range(DEVICES - 1)]


def stream_kernel(axis, rows, x_hbm, w_hbm, b_hbm, cand_hbm, t_hbm, emb_hbm, z_ref, norm_ref, candz_ref,
                  ebuf, et_ref, x_ref, w_ref, b_ref, cand_ref, t_ref, a_ref, m_ref, s_ref, q_ref, q_recv, st_ref, st_recv,
                  ecopy_sem, in_sem, q_sem, st_sem):
    width = x_ref.shape[1]
    chunks = rows // CHUNK
    inputs = [pltpu.make_async_copy(src, dst, in_sem.at[n]) for n, (src, dst) in enumerate(
        [(x_hbm, x_ref), (w_hbm, w_ref), (b_hbm, b_ref), (cand_hbm, cand_ref), (t_hbm, t_ref)])]
    for copy in inputs:
        copy.start()

    groups = (chunks - SINGLES) // GROUP
    transfers = groups + SINGLES

    def fetch(n, single):
        first = (groups * GROUP + n - groups) * CHUNK if single else n * GROUP * CHUNK
        size = CHUNK if single else GROUP * CHUNK
        slot = lax.rem(n, SLOTS)
        return pltpu.make_async_copy(
            emb_hbm.at[pl.ds(first, size), :], ebuf.at[slot, pl.ds(0, size), :], ecopy_sem.at[slot])

    def begin(n):
        @pl.when(n < groups)
        def _():
            fetch(n, False).start()

        @pl.when((n >= groups) & (n < transfers))
        def _():
            fetch(n, True).start()

    for n in range(SLOTS):
        fetch(n, False).start()

    me = lax.axis_index(axis)
    peers = peers_of(me)
    barrier = pltpu.get_barrier_semaphore()
    for peer in peers:
        pl.semaphore_signal(barrier, inc=1, device_id=(peer,), device_id_type=MESH)

    for copy in inputs:
        copy.wait()
    x = x_ref[...].astype(jnp.float32)
    centered = x - jnp.mean(x, axis=-1, keepdims=True)
    var = jnp.mean(centered * centered, axis=-1, keepdims=True)
    scaled = centered * lax.rsqrt(var + 1e-5)
    gain, bias = w_ref[...].astype(jnp.float32), b_ref[...].astype(jnp.float32)
    for k in range(width // LANES):
        part = scaled[:, k * LANES:(k + 1) * LANES] * gain[k:k + 1, :] + bias[k:k + 1, :]
        a_ref[:, k * LANES:(k + 1) * LANES] = part.astype(jnp.bfloat16)
    m_ref[...] = jnp.full(m_ref.shape, -jnp.inf, jnp.float32)
    s_ref[...] = jnp.zeros(s_ref.shape, jnp.float32)
    q_ref[...] = jnp.zeros(q_ref.shape, jnp.float32)
    temp = t_ref[0]

    def logits(i, slot, dots):
        for n, (first, size, flip) in enumerate(dots):
            tile = ebuf[slot, first:first + size, :]
            if flip:
                et_ref[n] = tile.T
                z = jnp.dot(a_ref[...], et_ref[n], preferred_element_type=jnp.float32)
            else:
                z = lax.dot_general(tile, a_ref[...], (((1,), (1,)), ((), ())), preferred_element_type=jnp.float32).T
            z_ref[:, pl.ds(pl.multiple_of(i * CHUNK + first, LANES), size)] = z / temp

    def tiles_of(i):
        return [z_ref[:, pl.ds(pl.multiple_of(i * CHUNK + t, LANES), LANES)] for t in range(0, CHUNK, LANES)]

    def candidates(i):
        cand = cand_ref[...] - me * rows - i * CHUNK
        lane, group = jnp.bitwise_and(cand, LANES - 1), jnp.right_shift(cand, 7)
        q = q_ref[...]
        for k, z in enumerate(tiles_of(i)):
            q = jnp.where(group == k, jnp.take_along_axis(z, lane, axis=1, mode="promise_in_bounds"), q)
        q_ref[...] = q

    def statistics(i):
        tiles = tiles_of(i)
        old = m_ref[...]
        new = functools.reduce(jnp.maximum, tiles, old)
        total = s_ref[...] * jnp.exp(old - new)
        for z in tiles:
            total = total + jnp.exp(z - new)
        m_ref[...] = new
        s_ref[...] = total

    def fold(i):
        statistics(i)
        candidates(i)

    fetch(0, False).wait()
    logits(0, 0, GROUP_DOTS)

    @pl.loop(1, groups)
    def _(n):
        begin(n + SLOTS - 1)
        fetch(n, False).wait()
        for j in range(GROUP):
            fold((n - 1) * GROUP + j)
        logits(n * GROUP, lax.rem(n, SLOTS), GROUP_DOTS)

    for j in range(GROUP - 1):
        fold((groups - 1) * GROUP + j)

    @pl.loop(groups, transfers)
    def _(n):
        begin(n + SLOTS - 1)
        fetch(n, True).wait()
        i = groups * GROUP + n - groups
        fold(i - 1)
        logits(i, lax.rem(n, SLOTS), DOTS)

    pl.semaphore_wait(barrier, len(peers))
    candidates(chunks - 1)
    statistics(chunks - 1)
    m = m_ref[...]
    row_max = jnp.max(m, axis=1, keepdims=True)
    local = row_max + jnp.log(jnp.sum(s_ref[...] * jnp.exp(m - row_max), axis=1, keepdims=True))
    diagonal = lax.broadcasted_iota(jnp.int32, m.shape, 0) == lax.broadcasted_iota(jnp.int32, m.shape, 1)
    mine = jnp.sum(jnp.where(diagonal, local, 0.0), axis=0, keepdims=True)
    st_ref[...] = mine

    def send(src, dst, sems, peer):
        slot = me - (me - peer + DEVICES - 1) // DEVICES
        pltpu.make_async_remote_copy(
            src_ref=src, dst_ref=dst.at[slot], send_sem=sems.at[0], recv_sem=sems.at[1],
            device_id=(peer,), device_id_type=MESH).start()

    def all_of(buf, sems):
        return pltpu.make_async_remote_copy(
            src_ref=buf, dst_ref=buf, send_sem=sems.at[0], recv_sem=sems.at[1],
            device_id=(peers[0],), device_id_type=MESH)

    for peer in peers[:2]:
        send(st_ref, st_recv, st_sem, peer)
    for peer in peers[:2]:
        send(q_ref, q_recv, q_sem, peer)
    for peer in peers[2:]:
        send(st_ref, st_recv, st_sem, peer)
    for peer in peers[2:]:
        send(q_ref, q_recv, q_sem, peer)
    all_of(st_recv, st_sem).wait_recv()
    parts = [mine] + [st_recv[k] for k in range(len(peers))]
    top = functools.reduce(jnp.maximum, parts)
    norm = top + jnp.log(functools.reduce(jnp.add, [jnp.exp(p - top) for p in parts]))
    norm = jnp.sum(jnp.where(diagonal, norm, 0.0), axis=1, keepdims=True)
    norm_ref[...] = jnp.broadcast_to(norm, norm_ref.shape)
    all_of(q_recv, q_sem).wait_recv()
    candz_ref[...] = functools.reduce(jnp.add, [q_recv[k] for k in range(len(peers))], q_ref[...])
    all_of(st_recv, st_sem).wait_send()
    all_of(q_recv, q_sem).wait_send()


def finish_kernel(z_ref, norm_ref, candz_ref, lp_hbm, q_hbm, buf, q_ref, sem):
    norm = norm_ref[...]
    q_ref[...] = candz_ref[...] - norm
    copies, start = [pltpu.make_async_copy(q_ref, q_hbm, sem.at[len(PIECES)])], 0
    for n, size in enumerate(PIECES):
        for c in range(start, start + size, LANES):
            buf[:, c:c + LANES] = z_ref[:, c:c + LANES] - norm
        copies.append(pltpu.make_async_copy(buf.at[:, pl.ds(start, size)], lp_hbm.at[:, pl.ds(start, size)], sem.at[n]))
        copies[-1].start()
        start += size
        if n == 0:
            copies[0].start()
    for copy in copies:
        copy.wait()


def solution(mesh):
    axis = mesh.axis_names[0]

    def per_device(hidden, ln_weight, ln_bias, emb, temperature, cand_ids):
        batch, width = hidden.shape
        rows = emb.shape[0]
        vmem = pl.BlockSpec(memory_space=pltpu.VMEM)
        hbm = pl.BlockSpec(memory_space=pl.ANY)
        f32, bf16 = jnp.float32, jnp.bfloat16
        dma = pltpu.SemaphoreType.DMA
        block = (width // LANES, LANES)
        small = [hidden, ln_weight.reshape(block), ln_bias.reshape(block), cand_ids, temperature.reshape(1)]
        small = [pltpu.with_memory_space_constraint(v, pltpu.HBM) for v in small[:4]] + small[4:]
        z, norm, candz = pl.pallas_call(
            functools.partial(stream_kernel, axis, rows),
            out_shape=(pltpu.VMEM((batch, rows), f32), pltpu.VMEM((batch, LANES), f32),
                       pltpu.VMEM((batch, LANES), f32)),
            in_specs=[hbm] * 6,
            out_specs=(vmem, vmem, vmem),
            scratch_shapes=[
                pltpu.VMEM((SLOTS, GROUP * CHUNK, width), bf16),
                pltpu.VMEM((len(GROUP_DOTS), width, 256), bf16),
                pltpu.VMEM((batch, width), bf16),
                pltpu.VMEM(block, bf16),
                pltpu.VMEM(block, bf16),
                pltpu.VMEM((batch, LANES), jnp.int32),
                pltpu.SMEM((1,), f32),
                pltpu.VMEM((batch, width), bf16),
                pltpu.VMEM((batch, LANES), f32),
                pltpu.VMEM((batch, LANES), f32),
                pltpu.VMEM((batch, LANES), f32),
                pltpu.VMEM((DEVICES - 1, batch, LANES), f32),
                pltpu.VMEM((1, LANES), f32),
                pltpu.VMEM((DEVICES - 1, 1, LANES), f32),
                dma((SLOTS,)), dma((5,)), dma((2,)), dma((2,)),
            ],
            compiler_params=pltpu.CompilerParams(
                collective_id=0, has_side_effects=True, vmem_limit_bytes=52 * 1024 * 1024),
        )(*small, emb)
        return pl.pallas_call(
            finish_kernel,
            out_shape=(jax.ShapeDtypeStruct((batch, rows), f32), jax.ShapeDtypeStruct((batch, LANES), f32)),
            in_specs=[vmem, vmem, vmem],
            out_specs=(hbm, hbm),
            scratch_shapes=[pltpu.VMEM((batch, rows), f32), pltpu.VMEM((batch, LANES), f32),
                            dma((len(PIECES) + 1,))],
            compiler_params=pltpu.CompilerParams(vmem_limit_bytes=16 * 1024 * 1024),
        )(z, norm, candz)

    return jax.shard_map(
        per_device,
        mesh=mesh,
        in_specs=(P(), P(), P(), P(axis, None), P(), P()),
        out_specs=(P(None, axis), P()),
        check_vma=False,
    )
```
